32 devices in a mesh: shard: 32 (over z, y, x, core).
Axes of the slice: x: 2, y: 2, z: 4, core: 2. Of those that a mesh axis runs over, the one named last changes fastest.
Arguments:
- lookup_ids: int32 [8192, 4, 8], P('shard'), may hold values from 0 to 131071, as said below
- bag_lengths: int32 [8192, 4], P('shard'), may hold values from 1 to 8
- pooled_gradients: bfloat16 [8192, 4, 128], P('shard'), may hold values from -6 to 6
- tables: float32 [4, 131072, 128], P(None, 'shard'), may hold values from -4 to 4
- accumulators: float32 [4, 131072], P(None, 'shard'), may hold values from 0.05 to 2
Outputs:
- new_tables: float32 [4, 131072, 128], P(None, 'shard')
- new_accumulators: float32 [4, 131072], P(None, 'shard')
- gradient_scale: float32 [], replicated
The draws below stay inside these ranges and needn't reach their ends.
Inputs may be any that keep to these rules, and one draw needn't show every extreme that they name: `lookup_ids`: row ids are rows 0 to 131071 of their table. Among the 256 x 8 entries of one table held by one device (padding positions included), the rows of every owning device's block of 4096 rows are named exactly 64 times. About half the lookups fall on the first 32 rows of an owner's block.
All inputs are finite; a program needn't handle non-finite values.
Results may differ from the reference program's by a relative error of at most 0.0003.
Values may be sent and summed in bfloat16 or wider, within the bound.
A program may use at most 128 MiB of HBM per device.

```python
import math
import jax
import jax.numpy as jnp
from jax import lax

E = 128
NT = 4
L = 8
HOT = 32
B_DEV = 256
ROWS_DEV = 4096
BATCH = 8192
ROWS = 131072


def draw_lookup_ids(key, part):
    peer_count = BATCH // B_DEV
    lookups = B_DEV * L

    def one_block(block_key):
        first_key, second_key, third_key, fourth_key = jax.random.split(block_key, 4)
        shuffled = jax.random.permutation(first_key, lookups)
        owners = shuffled % peer_count
        cold_rows = jax.random.randint(second_key, (lookups,), 0, ROWS_DEV)
        hot_rows = jax.random.randint(third_key, (lookups,), 0, min(HOT, ROWS_DEV))
        chooser = jax.random.randint(fourth_key, (lookups,), 0, 2)
        local_rows = jnp.where(chooser == 1, hot_rows, cold_rows)
        return (owners * ROWS_DEV + local_rows).astype(jnp.int32)
    block_keys = jax.random.split(jax.random.fold_in(key, 17), peer_count * NT)
    blocks = jax.vmap(one_block)(block_keys)
    blocks = blocks.reshape(peer_count, NT, B_DEV, L).transpose(0, 2, 1, 3)
    return blocks.reshape(BATCH, NT, L)


def touch_ends(array, key, low, high):
    dims = array.shape
    spot = [jax.random.randint(jax.random.fold_in(key, axis), (), 0, dims[axis]) for axis in range(len(dims))]
    array = array.at[tuple(spot)].set(low)
    longest = dims.index(max(dims))
    spot[longest] = (spot[longest] + 1) % dims[longest]
    return array.at[tuple(spot)].set(high)


def block_scale(stream_key, dims, shards, low, largest):
    def one(dim, blocks):
        steps = jax.random.uniform(jax.random.fold_in(jax.random.fold_in(stream_key, 6), dim), (blocks,), jnp.float32, low / len(shards), largest / len(shards))
        return jnp.repeat(jnp.exp(steps), dims[dim] // blocks).reshape((-1,) + (1,) * (len(dims) - dim - 1))

    level = one(*shards[0])
    for cut in shards[1:]:
        level = level * one(*cut)
    return level


def bell_draw(stream_key, dims, width, most, shards=(), kind=jnp.bfloat16):
    loudness = block_scale(stream_key, dims, shards, -0.22, 0.18) if shards else 1.0
    array = jax.random.normal(stream_key, dims, jnp.float32) * width * loudness
    return jnp.minimum(jnp.maximum(array, -most), most).astype(kind)


def setup_inputs(seed: int = 0) -> dict:
    key_list = jax.random.split(jax.random.key(seed), 6)
    lookup_ids = draw_lookup_ids(jax.random.fold_in(key_list[5], 71), 0)
    bag_lengths = touch_ends(jax.random.randint(key_list[1], (BATCH, NT), 1, L + 1), jax.random.fold_in(key_list[1], 1), 1, L).astype(jnp.int32)
    pooled_gradients = bell_draw(key_list[2], (BATCH, NT, E), 1.0, 6.0, ((0, 32),))
    tables = bell_draw(key_list[3], (NT, ROWS, E), 0.5, 4.0, ((1, 32),), jnp.float32)
    accumulators = jnp.clip(jnp.exp(math.log(2.0) - 3.6888794 * jax.random.uniform(key_list[4], (NT, ROWS), jnp.float32) ** block_scale(key_list[4], (NT, ROWS), ((1, 32),), -0.2, 0.2)), 0.05, 2.0)
    return {"lookup_ids": lookup_ids, "bag_lengths": bag_lengths, "pooled_gradients": pooled_gradients, "tables": tables, "accumulators": accumulators}


step_size = 0.5
epsilon = 1e-08

def reference(lookup_ids, bag_lengths, pooled_gradients, tables, accumulators):
    position = jnp.arange(L, dtype=jnp.int32)
    inside = position[None, None, :] < bag_lengths[:, :, None]
    scaled = (pooled_gradients.astype(jnp.float32) / bag_lengths[:, :, None].astype(jnp.float32)).astype(jnp.bfloat16)
    scaled = lax.optimization_barrier(scaled).astype(jnp.float32)

    def per_table(pieces):
        rows_here, inside_here, scaled_here, table_here, accum_here = pieces
        terms = jnp.where(inside_here[:, :, None], scaled_here[:, None, :], jnp.float32(0.0)).reshape(-1, E)
        summed = jax.ops.segment_sum(terms, rows_here.reshape(-1).astype(jnp.int32), num_segments=ROWS)
        mean_square = lax.optimization_barrier(jnp.mean(summed * summed, axis=1))
        new_accum = accum_here + mean_square
        new_table = table_here - step_size * summed / (jnp.sqrt(new_accum)[:, None] + epsilon)
        return (new_table, new_accum, jnp.sum(summed * summed))
    pieces = (lookup_ids.transpose(1, 0, 2), inside.transpose(1, 0, 2), scaled.transpose(1, 0, 2), tables, accumulators)
    new_tables, new_accumulators, squares = lax.map(per_table, pieces)
    gradient_scale = jnp.sqrt(jnp.sum(squares) / (E * NT * BATCH * L))
    return (new_tables, new_accumulators, gradient_scale)
```

```python
import functools

import jax
import jax.numpy as jnp
from jax import lax
from jax.experimental import pallas as pl
from jax.experimental.pallas import tpu as pltpu
from jax.sharding import PartitionSpec as P

step_size = 0.5
epsilon = 1e-08
MESH = pl.DeviceIdType.MESH
NT_DIMS = (((1,), (1,)), ((), ()))
DIGIT = 64


def arrange_kernel(peers, bucket, rows_dev, ids_ref, enc_ref, scaled_ref, terms_ref, rows_ref):
    count_tables, bag_width, samples = ids_ref.shape
    f32, bf16 = jnp.float32, jnp.bfloat16
    tri = (
        lax.broadcasted_iota(jnp.int32, (samples, samples), 0)
        < lax.broadcasted_iota(jnp.int32, (samples, samples), 1)
    ).astype(f32).astype(bf16)
    for t in range(count_tables):
        running = jnp.zeros((peers, 1), f32)
        info_t = jnp.zeros((bucket, peers), f32)
        high = jnp.zeros((peers, bucket), f32)
        low = jnp.zeros((peers, bucket), f32)
        for l in range(bag_width):
            ids = ids_ref[t, l : l + 1, :]
            owner = ids // rows_dev
            local = ids - owner * rows_dev
            hi = local // DIGIT
            lo = local - hi * DIGIT
            own = (lax.broadcasted_iota(jnp.int32, (peers, samples), 0) == owner).astype(f32)
            own_b = own.astype(bf16)
            before = jnp.dot(own_b, tri, preferred_element_type=f32) + running
            rank = jnp.sum(before * own, axis=0, keepdims=True).astype(jnp.int32)
            running = running + jnp.sum(own, axis=1, keepdims=True)
            at_rank = (
                (lax.broadcasted_iota(jnp.int32, (bucket, samples), 0) == rank)
                .astype(f32)
                .astype(bf16)
            )
            enc = enc_ref[t, l : l + 1, :].astype(f32)
            info_t += lax.dot_general(
                at_rank, (own * enc).astype(bf16), NT_DIMS, preferred_element_type=f32
            )
            high += lax.dot_general(
                (own * hi.astype(f32)).astype(bf16), at_rank, NT_DIMS, preferred_element_type=f32
            )
            low += lax.dot_general(
                (own * lo.astype(f32)).astype(bf16), at_rank, NT_DIMS, preferred_element_type=f32
            )
        rows_ref[:, t, :] = (high * DIGIT + low).astype(jnp.int32)
        info_i = info_t.astype(jnp.int32)
        lane = lax.broadcasted_iota(jnp.int32, (bucket, samples), 1)
        group = min(peers, 8)
        for g in range(0, peers, group):
            pick = jnp.concatenate(
                [
                    (lane == info_i[:, o : o + 1]).astype(f32).astype(bf16)
                    for o in range(g, g + group)
                ],
                axis=0,
            )
            moved = jnp.dot(pick, scaled_ref[t], preferred_element_type=f32).astype(bf16)
            for o in range(group):
                terms_ref[g + o, t * bucket : (t + 1) * bucket, :] = moved[
                    o * bucket : (o + 1) * bucket
                ]


def exchange_kernel(n, terms_ref, rows_ref, got_ref, got_rows_ref, send, recv, rsend, rrecv, local):
    me = lax.axis_index("shard")
    barrier = pltpu.get_barrier_semaphore()

    @pl.loop(1, n)
    def _(i):
        pl.semaphore_signal(
            barrier, inc=1, device_id=(lax.rem(me + i, n),), device_id_type=MESH
        )

    own = pltpu.make_async_copy(terms_ref.at[me], got_ref.at[0], local.at[0])
    own.start()
    own_rows = pltpu.make_async_copy(rows_ref.at[me], got_rows_ref.at[0], local.at[1])
    own_rows.start()
    pl.semaphore_wait(barrier, n - 1)

    def copies(i):
        peer = lax.rem(me + i, n)
        return (
            pltpu.make_async_remote_copy(
                src_ref=rows_ref.at[peer],
                dst_ref=got_rows_ref.at[i],
                send_sem=rsend.at[i],
                recv_sem=rrecv.at[i],
                device_id=(peer,),
                device_id_type=MESH,
            ),
            pltpu.make_async_remote_copy(
                src_ref=terms_ref.at[peer],
                dst_ref=got_ref.at[i],
                send_sem=send.at[i],
                recv_sem=recv.at[i],
                device_id=(peer,),
                device_id_type=MESH,
            ),
        )

    @pl.loop(1, n)
    def _(i):
        for copy in copies(i):
            copy.start()

    own.wait()
    own_rows.wait()

    @pl.loop(1, n)
    def _(i):
        for copy in copies(i):
            copy.wait()


def update_kernel(parts, rows_ref, terms_ref, tables_ref, accum_ref, new_t_ref, new_a_ref, sq_ref):
    f32, bf16 = jnp.float32, jnp.bfloat16
    peers, bucket, width = terms_ref.shape
    count = peers * bucket
    part_rows = tables_ref.shape[2]
    rows = rows_ref[0]
    part = rows // part_rows
    within = rows - part * part_rows
    terms = terms_ref[...].reshape(count, width)
    part_f = part.astype(f32)
    columns = []
    for c in range(0, count, 128):
        columns.append(jnp.broadcast_to(part_f[:, c : c + 128], (128, 128)).T)
    part_col = jnp.concatenate(columns, axis=0)
    wide = jnp.concatenate(
        [
            jnp.where(part_col == q, terms.astype(f32), 0.0).astype(bf16)
            for q in range(parts)
        ],
        axis=1,
    )
    chunk = min(512, part_rows)
    total = jnp.zeros((8, width), f32)
    for m in range(0, part_rows, chunk):
        hot = (
            (lax.broadcasted_iota(jnp.int32, (chunk, count), 0) + m == within)
            .astype(f32)
            .astype(bf16)
        )
        summed = jnp.dot(hot, wide, preferred_element_type=f32)
        for q in range(parts):
            for r in range(0, chunk, 128):
                s = summed[r : r + 128, q * width : (q + 1) * width]
                square = s * s
                total += jnp.sum(square.reshape(16, 8, width), axis=0)
                mean = jnp.sum(square.T, axis=0, keepdims=True) * (1.0 / width)
                line = (m + r) // 128
                new_a = accum_ref[0, q, line : line + 1, :] + mean
                new_a_ref[0, q, line : line + 1, :] = new_a
                factor = step_size / (jnp.sqrt(new_a) + epsilon)
                spread = jnp.broadcast_to(factor, (128, 128)).T
                new_t_ref[0, q, m + r : m + r + 128, :] = (
                    tables_ref[0, q, m + r : m + r + 128, :] - s * spread
                )

    @pl.when(pl.program_id(0) == 0)
    def _():
        sq_ref[...] = jnp.zeros_like(sq_ref)

    sq_ref[...] += total


def scale_kernel(n, inverse, sq_ref, out_ref, got, send, recv):
    me = lax.axis_index("shard")
    barrier = pltpu.get_barrier_semaphore()

    @pl.loop(1, n)
    def _(i):
        pl.semaphore_signal(
            barrier, inc=1, device_id=(lax.rem(me + i, n),), device_id_type=MESH
        )

    pl.semaphore_wait(barrier, n - 1)

    def copy(i):
        peer = lax.rem(me + i, n)
        return pltpu.make_async_remote_copy(
            src_ref=sq_ref,
            dst_ref=got.at[i],
            send_sem=send.at[i],
            recv_sem=recv.at[i],
            device_id=(peer,),
            device_id_type=MESH,
        )

    @pl.loop(1, n)
    def _(i):
        copy(i).start()

    @pl.loop(1, n)
    def _(i):
        copy(i).wait()

    total = sq_ref[...] + jnp.sum(got[1:], axis=0)
    value = jnp.sum(jnp.sum(total, axis=1, keepdims=True), axis=0, keepdims=True)
    out_ref[...] = jnp.broadcast_to(jnp.sqrt(value * inverse), out_ref.shape)


def on_device(lookup_ids, bag_lengths, pooled_gradients, tables, accumulators):
    samples, count_tables, bag_width = lookup_ids.shape
    width = pooled_gradients.shape[2]
    rows_dev = tables.shape[1]
    n = lax.axis_size("shard")
    lookups = samples * bag_width
    bucket = lookups // n
    vmem = pl.BlockSpec(memory_space=pltpu.VMEM)
    anywhere = pl.BlockSpec(memory_space=pl.ANY)
    assert samples <= 256 and rows_dev <= 256 * DIGIT

    ids = lookup_ids.transpose(1, 2, 0)
    position = jnp.arange(bag_width, dtype=jnp.int32)
    sample = jnp.arange(samples, dtype=jnp.int32)
    inside = position[None, :, None] < bag_lengths.T[:, None, :]
    enc = jnp.where(inside, sample[None, None, :], -1)
    scaled = (
        (pooled_gradients.astype(jnp.float32) / bag_lengths[:, :, None].astype(jnp.float32))
        .astype(jnp.bfloat16)
        .transpose(1, 0, 2)
    )
    send_terms, send_rows = pl.pallas_call(
        functools.partial(arrange_kernel, n, bucket, rows_dev),
        out_shape=(
            jax.ShapeDtypeStruct((n, count_tables * bucket, width), jnp.bfloat16),
            jax.ShapeDtypeStruct((n, count_tables, bucket), jnp.int32),
        ),
        in_specs=[vmem] * 3,
        out_specs=(vmem, vmem),
    )(ids, enc, scaled)

    dma = pltpu.SemaphoreType.DMA
    got_terms, got_rows = pl.pallas_call(
        functools.partial(exchange_kernel, n),
        out_shape=(
            jax.ShapeDtypeStruct(send_terms.shape, jnp.bfloat16),
            jax.ShapeDtypeStruct(send_rows.shape, jnp.int32),
        ),
        in_specs=[vmem, vmem],
        out_specs=(vmem, vmem),
        scratch_shapes=[dma((n,)), dma((n,)), dma((n,)), dma((n,)), dma((2,))],
        compiler_params=pltpu.CompilerParams(collective_id=0, has_side_effects=True),
    )(send_terms, send_rows)
    table_rows = got_rows.transpose(1, 0, 2).reshape(count_tables, 1, lookups)

    parts = 4
    part_rows = rows_dev // parts
    lines = part_rows // 128
    new_tables, new_accumulators, squares = pl.pallas_call(
        functools.partial(update_kernel, parts),
        grid=(count_tables,),
        out_shape=(
            jax.ShapeDtypeStruct((count_tables, parts, part_rows, width), jnp.float32),
            jax.ShapeDtypeStruct((count_tables, parts, lines, 128), jnp.float32),
            jax.ShapeDtypeStruct((8, width), jnp.float32),
        ),
        in_specs=[
            pl.BlockSpec((1, 1, lookups), lambda t: (t, 0, 0)),
            pl.BlockSpec((n, bucket, width), lambda t: (0, t, 0)),
            pl.BlockSpec((1, parts, part_rows, width), lambda t: (t, 0, 0, 0)),
            pl.BlockSpec((1, parts, lines, 128), lambda t: (t, 0, 0, 0)),
        ],
        out_specs=(
            pl.BlockSpec((1, parts, part_rows, width), lambda t: (t, 0, 0, 0)),
            pl.BlockSpec((1, parts, lines, 128), lambda t: (t, 0, 0, 0)),
            pl.BlockSpec((8, width), lambda t: (0, 0)),
        ),
        compiler_params=pltpu.CompilerParams(vmem_limit_bytes=48 * 1024 * 1024),
    )(
        table_rows,
        got_terms,
        tables.reshape(count_tables, parts, part_rows, width),
        accumulators.reshape(count_tables, parts, lines, 128),
    )

    lookup_count = width * count_tables * lookups * n
    scale = pl.pallas_call(
        functools.partial(scale_kernel, n, 1.0 / lookup_count),
        out_shape=jax.ShapeDtypeStruct((8, 128), jnp.float32),
        in_specs=[vmem],
        out_specs=vmem,
        scratch_shapes=[
            pltpu.VMEM((n, 8, width), jnp.float32),
            dma((n,)),
            dma((n,)),
        ],
        compiler_params=pltpu.CompilerParams(collective_id=1, has_side_effects=True),
    )(squares)
    return (
        new_tables.reshape(tables.shape),
        new_accumulators.reshape(accumulators.shape),
        scale[0, 0],
    )


def solution(mesh):
    return jax.shard_map(
        on_device,
        mesh=mesh,
        in_specs=(
            P("shard", None, None),
            P("shard", None),
            P("shard", None, None),
            P(None, "shard", None),
            P(None, "shard"),
        ),
        out_specs=(P(None, "shard", None), P(None, "shard"), P()),
        check_vma=False,
    )
```

```python
import functools

import jax
import jax.numpy as jnp
from jax import lax
from jax.experimental import pallas as pl
from jax.experimental.pallas import tpu as pltpu
from jax.sharding import PartitionSpec as P

step_size = 0.5
epsilon = 1e-08
MESH = pl.DeviceIdType.MESH
NT_DIMS = (((1,), (1,)), ((), ()))
DIGIT = 64


def arrange_kernel(peers, bucket, rows_dev, ids_ref, enc_ref, scaled_ref, terms_ref, rows_ref):
    count_tables, bag_width, samples = ids_ref.shape
    f32, bf16 = jnp.float32, jnp.bfloat16
    tri = (
        lax.broadcasted_iota(jnp.int32, (samples, samples), 0)
        < lax.broadcasted_iota(jnp.int32, (samples, samples), 1)
    ).astype(f32).astype(bf16)
    for t in range(count_tables):
        running = jnp.zeros((peers, 1), f32)
        info_t = jnp.zeros((bucket, peers), f32)
        high = jnp.zeros((peers, bucket), f32)
        low = jnp.zeros((peers, bucket), f32)
        for l in range(bag_width):
            ids = ids_ref[t, l : l + 1, :]
            owner = ids // rows_dev
            local = ids - owner * rows_dev
            hi = local // DIGIT
            lo = local - hi * DIGIT
            own = (lax.broadcasted_iota(jnp.int32, (peers, samples), 0) == owner).astype(f32)
            own_b = own.astype(bf16)
            before = jnp.dot(own_b, tri, preferred_element_type=f32) + running
            rank = jnp.sum(before * own, axis=0, keepdims=True).astype(jnp.int32)
            running = running + jnp.sum(own, axis=1, keepdims=True)
            at_rank = (
                (lax.broadcasted_iota(jnp.int32, (bucket, samples), 0) == rank)
                .astype(f32)
                .astype(bf16)
            )
            enc = enc_ref[t, l : l + 1, :].astype(f32)
            info_t += lax.dot_general(
                at_rank, (own * enc).astype(bf16), NT_DIMS, preferred_element_type=f32
            )
            high += lax.dot_general(
                (own * hi.astype(f32)).astype(bf16), at_rank, NT_DIMS, preferred_element_type=f32
            )
            low += lax.dot_general(
                (own * lo.astype(f32)).astype(bf16), at_rank, NT_DIMS, preferred_element_type=f32
            )
        rows_ref[:, t, :] = (high * DIGIT + low).astype(jnp.int32)
        info_i = info_t.astype(jnp.int32)
        lane = lax.broadcasted_iota(jnp.int32, (bucket, samples), 1)
        group = min(peers, 8)
        for g in range(0, peers, group):
            pick = jnp.concatenate(
                [
                    (lane == info_i[:, o : o + 1]).astype(f32).astype(bf16)
                    for o in range(g, g + group)
                ],
                axis=0,
            )
            moved = jnp.dot(pick, scaled_ref[t], preferred_element_type=f32).astype(bf16)
            terms_ref[t, g : g + group] = moved.reshape(group, bucket, moved.shape[1])


def exchange_kernel(
    n, inverse, terms_ref, rows_ref, summed_ref, scale_ref,
    got, got_rows, squares, got_squares, send, recv, local,
):
    f32, bf16 = jnp.float32, jnp.bfloat16
    count_tables, parts, part_rows, width = summed_ref.shape
    bucket = rows_ref.shape[2]
    count = n * bucket
    me = lax.axis_index("shard")
    barrier = pltpu.get_barrier_semaphore()

    @pl.loop(1, n)
    def _(i):
        pl.semaphore_signal(
            barrier, inc=1, device_id=(lax.rem(me + i, n),), device_id_type=MESH
        )

    own = [
        pltpu.make_async_copy(terms_ref.at[t, me], got.at[t, 0], local.at[t])
        for t in range(count_tables)
    ]
    own.append(pltpu.make_async_copy(rows_ref.at[me], got_rows.at[0], local.at[count_tables]))
    for copy in own:
        copy.start()
    pl.semaphore_wait(barrier, n - 1)

    def start(source, target, i, k):
        pltpu.make_async_remote_copy(
            src_ref=source,
            dst_ref=target,
            send_sem=send.at[k],
            recv_sem=recv.at[k],
            device_id=(lax.rem(me + i, n),),
            device_id_type=MESH,
        ).start()

    def drain(target, sem):
        others = target.at[pl.ds(1, n - 1)]
        pltpu.make_async_copy(others, others, sem).wait()

    @pl.loop(1, n)
    def _(i):
        start(rows_ref.at[lax.rem(me + i, n)], got_rows.at[i], i, count_tables)

    for t in range(count_tables):

        @pl.loop(1, n)
        def _(i):
            start(terms_ref.at[t, lax.rem(me + i, n)], got.at[t, i], i, t)

    own[-1].wait()
    drain(got_rows, recv.at[count_tables])
    chunk = min(512, part_rows)
    total = jnp.zeros((8, width), f32)
    for t in range(count_tables):
        rows = jnp.concatenate([got_rows[i, t : t + 1, :] for i in range(n)], axis=1)
        part = rows // part_rows
        within = rows - part * part_rows
        part_f = part.astype(f32)
        part_col = jnp.concatenate(
            [
                jnp.broadcast_to(part_f[:, c : c + 128], (128, 128)).T
                for c in range(0, count, 128)
            ],
            axis=0,
        )
        own[t].wait()
        drain(got.at[t], recv.at[t])
        terms = got[t].reshape(count, width).astype(f32)
        wide = jnp.concatenate(
            [jnp.where(part_col == q, terms, 0.0).astype(bf16) for q in range(parts)], axis=1
        )
        for m in range(0, part_rows, chunk):
            hot = (
                (lax.broadcasted_iota(jnp.int32, (chunk, count), 0) + m == within)
                .astype(f32)
                .astype(bf16)
            )
            summed = jnp.dot(hot, wide, preferred_element_type=f32)
            for q in range(parts):
                s = summed[:, q * width : (q + 1) * width]
                summed_ref[t, q, m : m + chunk, :] = s
                total += jnp.sum((s * s).reshape(chunk // 8, 8, width), axis=0)
    squares[...] = total
    for t in range(count_tables):
        drain(got.at[t], send.at[t])
    drain(got_rows, send.at[count_tables])

    @pl.loop(1, n)
    def _(i):
        start(squares, got_squares.at[i], i, count_tables + 1)

    drain(got_squares, recv.at[count_tables + 1])
    total = squares[...] + jnp.sum(got_squares[1:], axis=0)
    value = jnp.sum(jnp.sum(total, axis=1, keepdims=True), axis=0, keepdims=True)
    scale_ref[...] = jnp.broadcast_to(jnp.sqrt(value * inverse), scale_ref.shape)
    drain(got_squares, send.at[count_tables + 1])


def update_kernel(summed_ref, tables_ref, accum_ref, new_t_ref, new_a_ref):
    parts, part_rows, width = tables_ref.shape[1:]
    table, part = pl.program_id(0), pl.program_id(1)
    for q in range(parts):
        for r in range(0, part_rows, 128):
            s = summed_ref[table, part, r : r + 128, :]
            mean = jnp.sum((s * s).T, axis=0, keepdims=True) * (1.0 / width)
            line = r // 128
            new_a = accum_ref[0, q, line : line + 1, :] + mean
            new_a_ref[0, q, line : line + 1, :] = new_a
            factor = step_size / (jnp.sqrt(new_a) + epsilon)
            spread = jnp.broadcast_to(factor, (128, 128)).T
            new_t_ref[0, q, r : r + 128, :] = tables_ref[0, q, r : r + 128, :] - s * spread


def on_device(lookup_ids, bag_lengths, pooled_gradients, tables, accumulators):
    samples, count_tables, bag_width = lookup_ids.shape
    width = pooled_gradients.shape[2]
    rows_dev = tables.shape[1]
    n = lax.axis_size("shard")
    lookups = samples * bag_width
    bucket = lookups // n
    vmem = pl.BlockSpec(memory_space=pltpu.VMEM)
    assert samples <= 256 and rows_dev <= 256 * DIGIT

    ids = lookup_ids.transpose(1, 2, 0)
    position = jnp.arange(bag_width, dtype=jnp.int32)
    sample = jnp.arange(samples, dtype=jnp.int32)
    inside = position[None, :, None] < bag_lengths.T[:, None, :]
    enc = jnp.where(inside, sample[None, None, :], -1)
    scaled = (
        (pooled_gradients.astype(jnp.float32) / bag_lengths[:, :, None].astype(jnp.float32))
        .astype(jnp.bfloat16)
        .transpose(1, 0, 2)
    )
    send_terms, send_rows = pl.pallas_call(
        functools.partial(arrange_kernel, n, bucket, rows_dev),
        out_shape=(
            jax.ShapeDtypeStruct((count_tables, n, bucket, width), jnp.bfloat16),
            jax.ShapeDtypeStruct((n, count_tables, bucket), jnp.int32),
        ),
        in_specs=[vmem] * 3,
        out_specs=(vmem, vmem),
        compiler_params=pltpu.CompilerParams(vmem_limit_bytes=16 * 1024 * 1024),
    )(ids, enc, scaled)

    parts = 4
    part_rows = rows_dev // parts
    lines = part_rows // 128
    lookup_count = width * count_tables * lookups * n
    dma = pltpu.SemaphoreType.DMA
    summed, scale = pl.pallas_call(
        functools.partial(exchange_kernel, n, 1.0 / lookup_count),
        out_shape=(
            jax.ShapeDtypeStruct((count_tables, parts, part_rows, width), jnp.float32),
            jax.ShapeDtypeStruct((8, 128), jnp.float32),
        ),
        in_specs=[vmem, vmem],
        out_specs=(vmem, vmem),
        scratch_shapes=[
            pltpu.VMEM((count_tables, n, bucket, width), jnp.bfloat16),
            pltpu.VMEM((n, count_tables, bucket), jnp.int32),
            pltpu.VMEM((8, width), jnp.float32),
            pltpu.VMEM((n, 8, width), jnp.float32),
            dma((count_tables + 2,)),
            dma((count_tables + 2,)),
            dma((count_tables + 1,)),
        ],
        compiler_params=pltpu.CompilerParams(
            collective_id=0, has_side_effects=True, vmem_limit_bytes=24 * 1024 * 1024
        ),
        cost_estimate=pl.CostEstimate(
            flops=2 * count_tables * lookups * rows_dev * width,
            bytes_accessed=32 * count_tables * lookups * width * 2,
            transcendentals=0,
        ),
    )(send_terms, send_rows)

    block = pl.BlockSpec((1, 1, part_rows, width), lambda t, q: (t, q, 0, 0))
    line_block = pl.BlockSpec((1, 1, lines, 128), lambda t, q: (t, q, 0, 0))
    new_tables, new_accumulators = pl.pallas_call(
        update_kernel,
        grid=(count_tables, parts),
        out_shape=(
            jax.ShapeDtypeStruct((count_tables, parts, part_rows, width), jnp.float32),
            jax.ShapeDtypeStruct((count_tables, parts, lines, 128), jnp.float32),
        ),
        in_specs=[vmem, block, line_block],
        out_specs=(block, line_block),
        compiler_params=pltpu.CompilerParams(vmem_limit_bytes=12 * 1024 * 1024),
    )(
        summed,
        tables.reshape(count_tables, parts, part_rows, width),
        accumulators.reshape(count_tables, parts, lines, 128),
    )
    return (
        new_tables.reshape(tables.shape),
        new_accumulators.reshape(accumulators.shape),
        scale[0, 0],
    )


def solution(mesh):
    return jax.shard_map(
        on_device,
        mesh=mesh,
        in_specs=(
            P("shard", None, None),
            P("shard", None),
            P("shard", None, None),
            P(None, "shard", None),
            P(None, "shard"),
        ),
        out_specs=(P(None, "shard", None), P(None, "shard"), P()),
        check_vma=False,
    )
```
